512 devices in a mesh: seq: 32 (over y, x), stretch: 16 (over z, core).
Axes of the slice: x: 4, y: 8, z: 8, core: 2. Of those that a mesh axis runs over, the one named last changes fastest.
Arguments:
- queries: bfloat16 [65536, 1792], P(('stretch', 'seq')), may hold values from -140 to 140
- keys: bfloat16 [65536, 256], P(('stretch', 'seq')), may hold values from -6 to 6
- values: bfloat16 [65536, 256], P(('stretch', 'seq')), may hold values from -6 to 6
Outputs:
- attended: bfloat16 [65536, 1792], P(('stretch', 'seq'))
The draws below stay inside these ranges and needn't reach their ends.
All inputs are finite; a program needn't handle non-finite values.
Results may differ from the reference program's by a relative error of at most 0.011.
Values may be sent and summed in bfloat16 or wider, within the bound.
No kernel may reach another device: no remote copies, remote signals or barrier semaphores. Data moves between devices by JAX's collectives and lax.ppermute only.
A program may use at most 64 MiB of HBM per device.

```python
import math
import jax
import jax.numpy as jnp
from jax import lax

QUERY_HEADS = 14
KEY_VALUE_HEADS = 2
HEAD_SIZE = 128
BLOCKS = 4
BLOCK_TOKENS = 4096
SEQS = 4
TOTAL_TOKENS = 65536


def base_keys(key):
    return jnp.clip(jax.random.normal(jax.random.fold_in(key, 11), (TOTAL_TOKENS, KEY_VALUE_HEADS * HEAD_SIZE), jnp.float32), -6.0, 6.0)


def draw_keys(key, part):
    rotary_base = base_keys(key)
    return rotary_base.astype(jnp.bfloat16)


def draw_queries(key, part):
    noise = 3.0 * jnp.clip(jax.random.normal(jax.random.fold_in(key, 17), (TOTAL_TOKENS, QUERY_HEADS * HEAD_SIZE), jnp.float32), -6.0, 6.0)
    return noise.astype(jnp.bfloat16)


def steps_of(key, dims, cuts, low, largest):
    gain = 1.0
    for position, parts in cuts:
        steps = jax.random.uniform(jax.random.fold_in(jax.random.fold_in(key, 6), position), (parts,), jnp.float32, low / len(cuts), largest / len(cuts))
        gain = gain * jnp.repeat(jnp.exp(steps), dims[position] // parts).reshape((-1,) + (1,) * (len(dims) - 1 - position))
    return gain


def bell_draw(stream_key, extent, width, most, cuts=(), kind=jnp.bfloat16):
    level = steps_of(stream_key, extent, cuts, -0.22, 0.18) if cuts else 1.0
    values = jax.random.normal(stream_key, extent, jnp.float32) * width * level
    return jnp.minimum(jnp.maximum(values, -most), most).astype(kind)


def setup_inputs(seed: int = 0) -> dict:
    key_of = jax.random.split(jax.random.key(seed), 4)
    return {
        "queries": draw_queries(jax.random.fold_in(key_of[3], 71), 0),
        "keys": draw_keys(jax.random.fold_in(key_of[3], 71), 0),
        "values": bell_draw(key_of[2], (TOTAL_TOKENS, KEY_VALUE_HEADS * HEAD_SIZE), 1.0, 6.0, ((0, 512),)),
    }


def apply_rotary(rows, token_positions, heads):
    half_width = HEAD_SIZE // 2
    inverse = 10000000.0 ** (-(jnp.arange(half_width, dtype=jnp.float32) * 2.0) / HEAD_SIZE)
    angles = token_positions.astype(jnp.float32)[:, None] * inverse[None, :]
    cosine = jnp.cos(angles)[:, None, :]
    sine_part = jnp.sin(angles)[:, None, :]
    shaped = rows.reshape(rows.shape[0], heads, HEAD_SIZE).astype(jnp.float32)
    first_half = shaped[..., :half_width]
    second_half = shaped[..., half_width:]
    turned = jnp.concatenate([first_half * cosine - second_half * sine_part, second_half * cosine + first_half * sine_part], axis=-1)
    return turned.reshape(rows.shape[0], heads * HEAD_SIZE).astype(jnp.bfloat16)

def reference(queries, keys, values):
    head_cluster = QUERY_HEADS // KEY_VALUE_HEADS
    score_scale = 1.0 / math.sqrt(HEAD_SIZE)
    rows_of_block = min(256, BLOCK_TOKENS)
    inner_position = jnp.arange(BLOCK_TOKENS, dtype=jnp.int32)
    outputs = [None] * (SEQS * BLOCKS)
    for sequence in range(SEQS):
        for block_position in range(BLOCKS):
            leading_row = (block_position * SEQS + sequence) * BLOCK_TOKENS
            query_rows = queries[leading_row:leading_row + BLOCK_TOKENS]
            rotated_sets = {'near': apply_rotary(query_rows, inner_position, QUERY_HEADS), 'next': apply_rotary(query_rows, inner_position + BLOCK_TOKENS, QUERY_HEADS), 'far': apply_rotary(query_rows, jnp.full((BLOCK_TOKENS,), 2 * BLOCK_TOKENS - 1, jnp.int32), QUERY_HEADS)}
            key_list = []
            value_list = []
            for source in range(block_position + 1):
                source_row = (source * SEQS + sequence) * BLOCK_TOKENS
                key_list.append(apply_rotary(keys[source_row:source_row + BLOCK_TOKENS], inner_position, KEY_VALUE_HEADS))
                value_list.append(values[source_row:source_row + BLOCK_TOKENS])
            rotated_keys = jnp.concatenate(key_list, axis=0).astype(jnp.float32).reshape(-1, KEY_VALUE_HEADS, HEAD_SIZE)
            rows_of_values = jnp.concatenate(value_list, axis=0).astype(jnp.float32).reshape(-1, KEY_VALUE_HEADS, HEAD_SIZE)

            def one_block(block_number, block_position=block_position, rotated_sets=rotated_sets, rotated_keys=rotated_keys, rows_of_values=rows_of_values):
                row_start = block_number * rows_of_block
                pieces = []
                for source in range(block_position + 1):
                    chosen = 'near' if source == block_position else 'next' if source == block_position - 1 else 'far'
                    block_of_query = lax.dynamic_slice_in_dim(rotated_sets[chosen], row_start, rows_of_block, 0)
                    block_of_query = block_of_query.astype(jnp.float32).reshape(rows_of_block, KEY_VALUE_HEADS, head_cluster, HEAD_SIZE)
                    key_block = rotated_keys[source * BLOCK_TOKENS:(source + 1) * BLOCK_TOKENS]
                    scores = jnp.einsum('rkgd,skd->kgrs', block_of_query, key_block, precision=lax.Precision.HIGHEST) * score_scale
                    if source == block_position:
                        allowed = (row_start + jnp.arange(rows_of_block, dtype=jnp.int32))[:, None] >= jnp.arange(BLOCK_TOKENS, dtype=jnp.int32)[None, :]
                        scores = jnp.where(allowed, scores, -1e+30)
                    pieces.append(scores)
                scores = jnp.concatenate(pieces, axis=-1)
                row_max = lax.optimization_barrier(jnp.max(scores, axis=-1, keepdims=True))
                weights = jnp.exp(scores - row_max)
                row_sum = lax.optimization_barrier(jnp.sum(weights, axis=-1))
                attended = jnp.einsum('kgrs,skd->rkgd', weights, rows_of_values, precision=lax.Precision.HIGHEST)
                attended = attended / jnp.transpose(row_sum, (2, 0, 1))[..., None]
                return attended.reshape(rows_of_block, QUERY_HEADS * HEAD_SIZE).astype(jnp.bfloat16)
            result = lax.map(one_block, jnp.arange(BLOCK_TOKENS // rows_of_block, dtype=jnp.int32))
            outputs[block_position * SEQS + sequence] = result.reshape(BLOCK_TOKENS, QUERY_HEADS * HEAD_SIZE)
    return jnp.concatenate(outputs, axis=0)
```

```python
import functools
import math

import jax
import jax.numpy as jnp
from jax import lax
from jax.experimental import pallas as pl
from jax.experimental.pallas import tpu as pltpu
from jax.sharding import PartitionSpec as P

QUERY_HEADS = 14
KEY_VALUE_HEADS = 2
HEAD_SIZE = 128
BLOCKS = 4
GROUP = QUERY_HEADS // KEY_VALUE_HEADS
ROWS = 128
STACKED = GROUP * ROWS
X = 4
Y = 8
SPAN = X * ROWS
EXPONENT = math.log2(math.e) / math.sqrt(HEAD_SIZE)
LOWEST = -1e30
CHUNK = 448


def worker(sequence, head, core):
    plane = 4 * (sequence % 2) + 2 * head + sequence // 2
    return 2 * plane + core


def stretch_pairs(which):
    pairs = []
    for sequence in range(4):
        for block in range(BLOCKS):
            head = (0 if block < 2 else 1) ^ which
            core = 0 if block in (0, 3) else 1
            pairs.append((4 * block + sequence, worker(sequence, head, core)))
    return pairs


def back(pairs):
    return [(b, a) for a, b in pairs]


def plane_shift(dx, dy):
    pairs = []
    for y in range(Y):
        for x in range(X):
            for g in range(16):
                target = ((y + dy) % Y) * X + (x + dx) % X
                pairs.append(((y * X + x) * 16 + g, target * 16 + g))
    return pairs


SWAP = [(i, i ^ 1) for i in range(16)]


def shifted(array, dx, dy):
    return lax.ppermute(array, ("seq", "stretch"), plane_shift(dx, dy))


def tables(positions):
    half = HEAD_SIZE // 2
    lane = jnp.arange(HEAD_SIZE, dtype=jnp.int32)
    inverse = 10000000.0 ** (-((lane % half).astype(jnp.float32) * 2.0) / HEAD_SIZE)
    angles = positions.astype(jnp.float32)[..., None] * inverse
    return jnp.cos(angles), jnp.where(lane < half, -jnp.sin(angles), jnp.sin(angles))


def spin(x, cosine, sine):
    return x * cosine + pltpu.roll(x, HEAD_SIZE // 2, 1) * sine


VMEM = pl.BlockSpec(memory_space=pltpu.VMEM)
SMEM = pl.BlockSpec(memory_space=pltpu.SMEM)


def key_kernel(key_ref, value_ref, cosine_ref, sine_ref, out_ref):
    cosine = cosine_ref[0]
    sine = sine_ref[0]
    for head in range(KEY_VALUE_HEADS):
        part = slice(head * HEAD_SIZE, (head + 1) * HEAD_SIZE)
        x = key_ref[:, part].astype(jnp.float32)
        out_ref[head, :, :HEAD_SIZE] = spin(x, cosine, sine).astype(jnp.bfloat16)
        out_ref[head, :, HEAD_SIZE:] = value_ref[:, part]


def query_kernel(where_ref, own_ref, other_ref, cosine_ref, sine_ref, out_ref):
    head = where_ref[0]
    core = where_ref[1]

    def turn(ref, which, kind, slot):
        cosine = cosine_ref[kind]
        sine = sine_ref[kind]
        for g in range(GROUP):
            x = ref[which, :, g * HEAD_SIZE : (g + 1) * HEAD_SIZE].astype(jnp.float32)
            out_ref[slot, g * ROWS : (g + 1) * ROWS, :] = spin(x, cosine, sine).astype(jnp.bfloat16)

    turn(own_ref, head, 0, 0)
    turn(own_ref, 1 - head, 0, 1)
    turn(other_ref, 1 - head, 2, 3)

    @pl.when(core == 0)
    def _():
        turn(other_ref, head, 1, 2)
        turn(own_ref, 1 - head, 2, 4)

    @pl.when(core == 1)
    def _():
        turn(own_ref, 1 - head, 1, 2)
        turn(other_ref, 1 - head, 1, 4)


def lanes(x, count):
    return [x[:, j * HEAD_SIZE : (j + 1) * HEAD_SIZE] for j in range(count)]


def absorb(query_ref, query, keys, values, acc_ref, top_ref, sum_ref, slot, limit):
    count = SPAN // HEAD_SIZE

    def score(c):
        part = query_ref[query, c * CHUNK : (c + 1) * CHUNK, :]
        return lax.dot_general(
            part, keys, (((1,), (1,)), ((), ())), preferred_element_type=jnp.float32
        )

    steps = STACKED // CHUNK
    coming = score(0)
    for c in range(steps):
        s = coming
        if c + 1 < steps:
            coming = score(c + 1)
        if limit is not None:
            row = lax.broadcasted_iota(jnp.int32, (CHUNK, SPAN), 0) + c * CHUNK
            s = jnp.where(limit[0] <= (row & (ROWS - 1)) + limit[1], s, LOWEST)
        rows = pl.ds(c * CHUNK, CHUNK)
        parts = lanes(s, count)
        highest = parts[0]
        for j in range(1, count):
            highest = jnp.maximum(highest, parts[j])
        before = top_ref[slot, rows, :]
        top = jnp.maximum(before, jnp.max(highest, axis=-1, keepdims=True))
        scaled = top * EXPONENT
        weights = [jnp.exp2(part * EXPONENT - scaled) for part in parts]
        fade = jnp.exp2(before * EXPONENT - scaled)
        total = weights[0]
        for j in range(1, count):
            total = total + weights[j]
        packed = jnp.concatenate([w.astype(jnp.bfloat16) for w in weights], axis=1)
        product = jnp.dot(packed, values, preferred_element_type=jnp.float32)
        top_ref[slot, rows, :] = top
        sum_ref[slot, rows, :] = sum_ref[slot, rows, :] * fade + total
        acc_ref[slot, rows, :] = acc_ref[slot, rows, :] * fade + product


def attend_kernel(first, last, offsets, where_ref, query_ref, *refs):
    number = len(offsets)
    block_refs = refs[:number]
    refs = refs[number:]
    if last:
        out_refs = refs[3:5]
        refs = refs[:3] + refs[5:]
    if not first:
        for source, target in zip(refs[:3], refs[3:6]):
            target[...] = source[...]
        refs = refs[3:]
    acc_ref, top_ref, sum_ref = refs[:3]
    core = where_ref[1]
    x = where_ref[2]
    y = where_ref[3]
    if first:
        acc_ref[...] = jnp.zeros_like(acc_ref)
        top_ref[...] = jnp.full_like(top_ref, LOWEST)
        sum_ref[...] = jnp.zeros_like(sum_ref)
    run = functools.partial(
        absorb, query_ref, acc_ref=acc_ref, top_ref=top_ref, sum_ref=sum_ref
    )
    for b in range(number):
        ref = block_refs[b]

        def columns(place, ref=ref):
            keys = ref[:, pl.ds(place, HEAD_SIZE)]
            values = ref[:, pl.ds(place + HEAD_SIZE, HEAD_SIZE)]
            return keys, values

        third = pl.multiple_of(core * (2 * HEAD_SIZE), HEAD_SIZE)
        keys, values = columns(0)
        run(query=2, keys=keys, values=values, slot=2 - core, limit=None)
        run(query=3, keys=keys, values=values, slot=3, limit=None)
        keys, values = columns(third)
        run(query=4, keys=keys, values=values, slot=1 + 2 * core, limit=None)
        if first:
            column = lax.broadcasted_iota(jnp.int32, (CHUNK, SPAN), 1)
            piece = column // ROWS
            place = jnp.zeros_like(column)
            for j, offset in enumerate((0, -1, 1, 2)):
                place = jnp.where(piece == j, (x + offset) & (X - 1), place)
            limit = (place * ROWS + (column & (ROWS - 1)), x * ROWS)
            for place, query in ((0, 0), (2 * HEAD_SIZE, 1)):
                keys, values = columns(place)
                run(query=query, keys=keys, values=values, slot=query, limit=limit)
        else:

            @pl.when(((y + offsets[b]) & (Y - 1)) < y)
            def _():
                for place, query in ((0, 0), (2 * HEAD_SIZE, 1)):
                    keys, values = columns(place)
                    run(query=query, keys=keys, values=values, slot=query, limit=None)

    if last:
        lane = lax.broadcasted_iota(jnp.int32, (STACKED, HEAD_SIZE), 1)
        for k in range(4):
            ref = out_refs[k // 2]
            total = jnp.sum(sum_ref[k], axis=-1, keepdims=True)
            ref[k % 2, :, :HEAD_SIZE] = acc_ref[k]
            ref[k % 2, :, HEAD_SIZE:] = jnp.where(lane < HEAD_SIZE // 2, top_ref[k], total)


def attend(where, query, blocks, offsets, state, first=False, last=False):
    number = len(blocks)
    block = jax.ShapeDtypeStruct((4, STACKED, HEAD_SIZE), jnp.float32)
    outs = [block] * 3
    if last:
        outs = [jax.ShapeDtypeStruct((2, STACKED, 2 * HEAD_SIZE), jnp.float32)] * 2
    flops = number * 4 * 4 * STACKED * SPAN * HEAD_SIZE
    return pl.pallas_call(
        functools.partial(attend_kernel, first, last, offsets),
        out_shape=outs,
        in_specs=[SMEM] + [VMEM] * (1 + number + len(state)),
        out_specs=[VMEM] * len(outs),
        scratch_shapes=[pltpu.VMEM(block.shape, block.dtype)] * 3 if last else [],
        cost_estimate=pl.CostEstimate(
            flops=flops, bytes_accessed=4 << 20, transcendentals=number * 4 * STACKED * SPAN
        ),
        compiler_params=pltpu.CompilerParams(vmem_limit_bytes=56 << 20),
        name="attend",
    )(where, query, *blocks, *state)


def merge_kernel(where_ref, own_ref, other_ref, out_ref):
    head = where_ref[0]
    for k in range(2):
        place = head if k == 0 else 1 - head
        for g in range(GROUP):
            rows = slice(g * ROWS, (g + 1) * ROWS)
            stats = other_ref[k, rows, HEAD_SIZE:]
            other_top = stats[:, :1]
            other_sum = stats[:, HEAD_SIZE - 1 :]
            own_stats = own_ref[k, rows, HEAD_SIZE:]
            top = own_stats[:, :1]
            highest = jnp.maximum(top, other_top)
            mine = jnp.exp2((top - highest) * EXPONENT)
            theirs = jnp.exp2((other_top - highest) * EXPONENT)
            total = own_stats[:, HEAD_SIZE - 1 :] * mine + other_sum * theirs
            value = own_ref[k, rows, :HEAD_SIZE] * mine + other_ref[k, rows, :HEAD_SIZE] * theirs
            out_ref[place, :, g * HEAD_SIZE : (g + 1) * HEAD_SIZE] = (value / total).astype(
                jnp.bfloat16
            )


def on_device(queries, keys, values):
    seq = lax.axis_index("seq")
    stretch = lax.axis_index("stretch")
    x = seq % X
    y = seq // X
    home_block = stretch // 4
    low = home_block < 2
    core = stretch % 2
    head = (stretch // 4) % 2
    positions = seq * ROWS + jnp.arange(ROWS, dtype=jnp.int32)
    length = ROWS * X * Y
    kind = jnp.arange(3, dtype=jnp.int32)[:, None]
    every = jnp.where(kind == 2, 2 * length - 1, positions[None, :] + kind * length)
    cosine, sine = tables(every)
    paired = pl.pallas_call(
        key_kernel,
        out_shape=jax.ShapeDtypeStruct((2, ROWS, 2 * HEAD_SIZE), jnp.bfloat16),
        in_specs=[VMEM] * 4,
        out_specs=VMEM,
        name="turn_keys",
    )(keys, values, cosine, sine)
    straight, crossed = stretch_pairs(0), stretch_pairs(1)

    def spread(first_half, second_half):
        one = lax.ppermute(jnp.where(low, first_half, second_half), "stretch", straight)
        two = lax.ppermute(jnp.where(low, second_half, first_half), "stretch", crossed)
        return one, two

    one, two = spread(paired[0], paired[1])
    swapped = head == 1
    own = jnp.concatenate(
        [jnp.where(swapped, two, one), jnp.where(swapped, one, two)], axis=1
    )
    half = GROUP * HEAD_SIZE
    query_one, query_two = spread(queries[:, :half], queries[:, half:])
    raw = jnp.stack([query_one, query_two])
    other_raw = lax.ppermute(raw, "stretch", SWAP)
    base = jnp.stack([head, core, x, y]).astype(jnp.int32)
    query = pl.pallas_call(
        query_kernel,
        out_shape=jax.ShapeDtypeStruct((5, STACKED, HEAD_SIZE), jnp.bfloat16),
        in_specs=[SMEM] + [VMEM] * 4,
        out_specs=VMEM,
        cost_estimate=pl.CostEstimate(flops=2 << 30, bytes_accessed=4 << 20, transcendentals=0),
        name="turn_queries",
    )(base, raw, other_raw, cosine, sine)

    right = shifted(own, 1, 0)
    left = shifted(own, -1, 0)
    far = shifted(own, 2, 0)
    row = jnp.concatenate([own, right, left, far], axis=0)
    row, query = lax.optimization_barrier((row, query))
    up, down = row, row
    blocks, offsets, state = [row], (0,), []
    for hop in range(1, Y // 2 + 1):
        next_up = shifted(up, 0, 1)
        next_down = shifted(down, 0, -1) if hop < Y // 2 else None
        state = attend(base, query, blocks, offsets, state, first=hop == 1)
        up, down, state = lax.optimization_barrier((next_up, next_down, state))
        blocks, offsets = [up, down], (-hop, hop)
    mine, send = attend(base, query, [up], (4,), state, last=True)
    received = lax.ppermute(send, "stretch", SWAP)
    merged = pl.pallas_call(
        merge_kernel,
        out_shape=jax.ShapeDtypeStruct((2, ROWS, half), jnp.bfloat16),
        in_specs=[SMEM] + [VMEM] * 2,
        out_specs=VMEM,
        compiler_params=pltpu.CompilerParams(vmem_limit_bytes=40 << 20),
        name="merge",
    )(base, mine, received)
    one = lax.ppermute(merged[0], "stretch", back(straight))
    two = lax.ppermute(merged[1], "stretch", back(crossed))
    return jnp.concatenate([jnp.where(low, one, two), jnp.where(low, two, one)], axis=1)


def solution(mesh):
    placed = P(("stretch", "seq"), None)
    return jax.shard_map(
        on_device,
        mesh=mesh,
        in_specs=(placed, placed, placed),
        out_specs=placed,
        check_vma=False,
    )
```

```python
import functools
import math

import jax
import jax.numpy as jnp
from jax import lax
from jax.experimental import pallas as pl
from jax.experimental.pallas import tpu as pltpu
from jax.sharding import PartitionSpec as P

QUERY_HEADS = 14
KEY_VALUE_HEADS = 2
HEAD_SIZE = 128
BLOCKS = 4
GROUP = QUERY_HEADS // KEY_VALUE_HEADS
ROWS = 128
STACKED = GROUP * ROWS
X = 4
Y = 8
SPAN = X * ROWS
EXPONENT = math.log2(math.e) / math.sqrt(HEAD_SIZE)
LOWEST = -1e30
CHUNK = 896


def worker(sequence, head, core):
    plane = 4 * (sequence % 2) + 2 * head + 1 - sequence // 2
    return 2 * plane + core


def stretch_pairs(which):
    pairs = []
    for sequence in range(4):
        for block in range(BLOCKS):
            head = (0 if block < 2 else 1) ^ which
            core = 0 if block in (0, 3) else 1
            pairs.append((4 * block + sequence, worker(sequence, head, core)))
    return pairs


def back(pairs):
    return [(b, a) for a, b in pairs]


def plane_shift(dx, dy):
    pairs = []
    for y in range(Y):
        for x in range(X):
            for g in range(16):
                target = ((y + dy) % Y) * X + (x + dx) % X
                pairs.append(((y * X + x) * 16 + g, target * 16 + g))
    return pairs


SWAP = [(i, i ^ 1) for i in range(16)]


def shifted(array, dx, dy):
    return lax.ppermute(array, ("seq", "stretch"), plane_shift(dx, dy))


def tables(positions):
    half = HEAD_SIZE // 2
    lane = jnp.arange(HEAD_SIZE, dtype=jnp.int32)
    inverse = 10000000.0 ** (-((lane % half).astype(jnp.float32) * 2.0) / HEAD_SIZE)
    angles = positions.astype(jnp.float32)[..., None] * inverse
    return jnp.cos(angles), jnp.where(lane < half, -jnp.sin(angles), jnp.sin(angles))


def spin(x, cosine, sine):
    return x * cosine + pltpu.roll(x, HEAD_SIZE // 2, 1) * sine


VMEM = pl.BlockSpec(memory_space=pltpu.VMEM)
SMEM = pl.BlockSpec(memory_space=pltpu.SMEM)


def unpack_kernel(where_ref, one_ref, two_ref, cosine_ref, sine_ref, out_ref, raw_ref):
    head = where_ref[0]
    cosine = cosine_ref[0]
    sine = sine_ref[0]
    for k, ref in enumerate((one_ref, two_ref)):
        slot = head ^ k
        place = pl.multiple_of(slot * (2 * HEAD_SIZE), 2 * HEAD_SIZE)
        x = ref[:, :HEAD_SIZE].astype(jnp.float32)
        out_ref[:, pl.ds(place, HEAD_SIZE)] = spin(x, cosine, sine).astype(jnp.bfloat16)
        out_ref[:, pl.ds(place + HEAD_SIZE, HEAD_SIZE)] = ref[:, HEAD_SIZE : 2 * HEAD_SIZE]
        raw_ref[slot] = ref[:, 2 * HEAD_SIZE :]


def query_kernel(where_ref, own_ref, other_ref, cosine_ref, sine_ref, out_ref):
    core = where_ref[1]

    def turn(ref, which, kind, slot):
        cosine = cosine_ref[kind]
        sine = sine_ref[kind]
        for g in range(GROUP):
            x = ref[which, :, g * HEAD_SIZE : (g + 1) * HEAD_SIZE].astype(jnp.float32)
            out_ref[slot, g * ROWS : (g + 1) * ROWS, :] = spin(x, cosine, sine).astype(jnp.bfloat16)

    turn(own_ref, 0, 0, 0)
    turn(own_ref, 1, 0, 1)
    turn(other_ref, 1, 2, 3)

    @pl.when(core == 0)
    def _():
        turn(other_ref, 0, 1, 2)
        turn(own_ref, 1, 2, 4)

    @pl.when(core == 1)
    def _():
        turn(own_ref, 1, 1, 2)
        turn(other_ref, 1, 1, 4)


def lanes(x, count):
    return [x[:, j * HEAD_SIZE : (j + 1) * HEAD_SIZE] for j in range(count)]


def absorb(query_ref, query, pairs, acc_ref, top_ref, sum_ref, slot, limit):
    def score(c):
        part = query_ref[query, c * CHUNK : (c + 1) * CHUNK, :]
        return [
            lax.dot_general(
                part, keys, (((1,), (1,)), ((), ())), preferred_element_type=jnp.float32
            )
            for keys, _ in pairs
        ]

    steps = STACKED // CHUNK
    coming = score(0)
    for c in range(steps):
        scores = coming
        if c + 1 < steps:
            coming = score(c + 1)
        if limit is not None:
            row = lax.broadcasted_iota(jnp.int32, (CHUNK, SPAN), 0) + c * CHUNK
            inside = limit[0] <= (row & (ROWS - 1)) + limit[1]
            scores = [jnp.where(inside, s, LOWEST) for s in scores]
        rows = pl.ds(c * CHUNK, CHUNK)
        parts = [part for s in scores for part in lanes(s, s.shape[1] // HEAD_SIZE)]
        highest = parts[0]
        for j in range(1, len(parts)):
            highest = jnp.maximum(highest, parts[j])
        before = top_ref[slot, rows, :]
        top = jnp.maximum(before, jnp.max(highest, axis=-1, keepdims=True))
        scaled = top * EXPONENT
        weights = [jnp.exp2(part * EXPONENT - scaled) for part in parts]
        fade = jnp.exp2(before * EXPONENT - scaled)
        total = weights[0]
        for j in range(1, len(parts)):
            total = total + weights[j]
        product = None
        used = 0
        for _, values in pairs:
            count = values.shape[0] // HEAD_SIZE
            some = weights[used : used + count]
            used += count
            packed = jnp.concatenate([w.astype(jnp.bfloat16) for w in some], axis=1)
            more = jnp.dot(packed, values, preferred_element_type=jnp.float32)
            product = more if product is None else product + more
        top_ref[slot, rows, :] = top
        sum_ref[slot, rows, :] = sum_ref[slot, rows, :] * fade + total
        acc_ref[slot, rows, :] = acc_ref[slot, rows, :] * fade + product


def attend_kernel(first, last, offsets, where_ref, query_ref, *refs):
    number = len(offsets)
    block_refs = refs[:number]
    refs = refs[number:]
    if last:
        out_refs = refs[3:5]
        refs = refs[:3] + refs[5:]
    if not first:
        for source, target in zip(refs[:3], refs[3:6]):
            target[...] = source[...]
        refs = refs[3:]
    acc_ref, top_ref, sum_ref = refs[:3]
    core = where_ref[1]
    x = where_ref[2]
    y = where_ref[3]
    if first:
        acc_ref[...] = jnp.zeros_like(acc_ref)
        top_ref[...] = jnp.full_like(top_ref, LOWEST)
        sum_ref[...] = jnp.zeros_like(sum_ref)
    run = functools.partial(
        absorb, query_ref, acc_ref=acc_ref, top_ref=top_ref, sum_ref=sum_ref
    )

    def columns(ref, place):
        keys = ref[:, pl.ds(place, HEAD_SIZE)]
        values = ref[:, pl.ds(place + HEAD_SIZE, HEAD_SIZE)]
        return keys, values

    def causal(ref, limit):
        def body(query, carry):
            place = pl.multiple_of(query * (2 * HEAD_SIZE), 2 * HEAD_SIZE)
            run(query=query, pairs=[columns(ref, place)], slot=query, limit=limit)
            return carry

        lax.fori_loop(0, 2, body, 0)

    third = pl.multiple_of(core * (2 * HEAD_SIZE), 2 * HEAD_SIZE)
    pairs = [columns(ref, 0) for ref in block_refs]
    run(query=2, pairs=pairs, slot=2 - core, limit=None)
    run(query=3, pairs=pairs, slot=3, limit=None)
    pairs = [columns(ref, third) for ref in block_refs]
    run(query=4, pairs=pairs, slot=1 + 2 * core, limit=None)
    if first:
        column = lax.broadcasted_iota(jnp.int32, (CHUNK, SPAN), 1)
        causal(block_refs[0], (column, x * ROWS))
    else:
        for b in range(number):

            @pl.when(((y + offsets[b]) & (Y - 1)) < y)
            def _(b=b):
                causal(block_refs[b], None)

    if last:
        lane = lax.broadcasted_iota(jnp.int32, (STACKED, HEAD_SIZE), 1)
        for k in range(4):
            ref = out_refs[k // 2]
            total = jnp.sum(sum_ref[k], axis=-1, keepdims=True)
            ref[k % 2, :, :HEAD_SIZE] = acc_ref[k]
            ref[k % 2, :, HEAD_SIZE:] = jnp.where(lane < HEAD_SIZE // 2, top_ref[k], total)


def attend(where, query, blocks, offsets, state, first=False, last=False):
    number = len(blocks)
    block = jax.ShapeDtypeStruct((4, STACKED, HEAD_SIZE), jnp.float32)
    outs = [block] * 3
    if last:
        outs = [jax.ShapeDtypeStruct((2, STACKED, 2 * HEAD_SIZE), jnp.float32)] * 2
    flops = number * 4 * 4 * STACKED * SPAN * HEAD_SIZE
    return pl.pallas_call(
        functools.partial(attend_kernel, first, last, offsets),
        out_shape=outs,
        in_specs=[SMEM] + [VMEM] * (1 + number + len(state)),
        out_specs=[VMEM] * len(outs),
        scratch_shapes=[pltpu.VMEM(block.shape, block.dtype)] * 3 if last else [],
        cost_estimate=pl.CostEstimate(
            flops=flops, bytes_accessed=4 << 20, transcendentals=number * 4 * STACKED * SPAN
        ),
        compiler_params=pltpu.CompilerParams(vmem_limit_bytes=24 << 20),
        name="attend",
    )(where, query, *blocks, *state)


def halves(stats):
    lane = lax.broadcasted_iota(jnp.int32, stats.shape, 1)
    turned = pltpu.roll(stats, HEAD_SIZE // 2, 1)
    left = lane < HEAD_SIZE // 2
    return jnp.where(left, stats, turned), jnp.where(left, turned, stats)


def merge_kernel(where_ref, own_ref, other_ref, out_ref):
    head = where_ref[0]
    for k in range(2):
        place = head if k == 0 else 1 - head
        for g in range(GROUP):
            rows = slice(g * ROWS, (g + 1) * ROWS)
            top, own_sum = halves(own_ref[k, rows, HEAD_SIZE:])
            other_top, other_sum = halves(other_ref[k, rows, HEAD_SIZE:])
            highest = jnp.maximum(top, other_top)
            mine = jnp.exp2((top - highest) * EXPONENT)
            theirs = jnp.exp2((other_top - highest) * EXPONENT)
            total = own_sum * mine + other_sum * theirs
            value = own_ref[k, rows, :HEAD_SIZE] * mine + other_ref[k, rows, :HEAD_SIZE] * theirs
            out_ref[place, :, g * HEAD_SIZE : (g + 1) * HEAD_SIZE] = (value / total).astype(
                jnp.bfloat16
            )


def on_device(queries, keys, values):
    seq = lax.axis_index("seq")
    stretch = lax.axis_index("stretch")
    x = seq % X
    y = seq // X
    home_block = stretch // 4
    low = home_block < 2
    core = stretch % 2
    head = (stretch // 4) % 2
    positions = seq * ROWS + jnp.arange(ROWS, dtype=jnp.int32)
    length = ROWS * X * Y
    kind = jnp.arange(3, dtype=jnp.int32)[:, None]
    every = jnp.where(kind == 2, 2 * length - 1, positions[None, :] + kind * length)
    cosine, sine = tables(every)
    base = jnp.stack([head, core, x, y]).astype(jnp.int32)
    straight, crossed = stretch_pairs(0), stretch_pairs(1)

    half = GROUP * HEAD_SIZE
    packs = [
        jnp.concatenate(
            [
                keys[:, k * HEAD_SIZE : (k + 1) * HEAD_SIZE],
                values[:, k * HEAD_SIZE : (k + 1) * HEAD_SIZE],
                queries[:, k * half : (k + 1) * half],
            ],
            axis=1,
        )
        for k in range(KEY_VALUE_HEADS)
    ]
    one = lax.ppermute(jnp.where(low, packs[0], packs[1]), "stretch", straight)
    two = lax.ppermute(jnp.where(low, packs[1], packs[0]), "stretch", crossed)
    own, raw = pl.pallas_call(
        unpack_kernel,
        out_shape=[
            jax.ShapeDtypeStruct((ROWS, 4 * HEAD_SIZE), jnp.bfloat16),
            jax.ShapeDtypeStruct((2, ROWS, half), jnp.bfloat16),
        ],
        in_specs=[SMEM] + [VMEM] * 4,
        out_specs=[VMEM] * 2,
        compiler_params=pltpu.CompilerParams(vmem_limit_bytes=8 << 20),
        name="unpack",
    )(base, one, two, cosine, sine)
    lines = [[X * line + k for k in range(X)] for line in range(Y)]
    row = lax.all_gather(own, "seq", axis=0, tiled=True, axis_index_groups=lines)
    row, raw = lax.optimization_barrier((row, raw))
    other_raw = lax.ppermute(raw, "stretch", SWAP)
    query = pl.pallas_call(
        query_kernel,
        out_shape=jax.ShapeDtypeStruct((5, STACKED, HEAD_SIZE), jnp.bfloat16),
        in_specs=[SMEM] + [VMEM] * 4,
        out_specs=VMEM,
        cost_estimate=pl.CostEstimate(flops=2 << 30, bytes_accessed=4 << 20, transcendentals=0),
        compiler_params=pltpu.CompilerParams(vmem_limit_bytes=12 << 20),
        name="turn_queries",
    )(base, raw, other_raw, cosine, sine)
    up, down = row, row
    blocks, offsets, state = [row], (0,), []
    for hop in range(1, Y // 2 + 1):
        if hop == Y // 2:
            up, down = up[: SPAN // 2], down[SPAN // 2 :]
        next_up = shifted(up, 0, 1)
        next_down = shifted(down, 0, -1)
        state = attend(base, query, blocks, offsets, state, first=hop == 1)
        up, _ = lax.optimization_barrier((next_up, state[2]))
        down, _ = lax.optimization_barrier((next_down, state[2]))
        blocks, offsets = [next_up, next_down], (-hop, hop)
    mine, send = attend(base, query, blocks, (4, 4), state, last=True)
    received = lax.ppermute(send, "stretch", SWAP)
    merged = pl.pallas_call(
        merge_kernel,
        out_shape=jax.ShapeDtypeStruct((2, ROWS, half), jnp.bfloat16),
        in_specs=[SMEM] + [VMEM] * 2,
        out_specs=VMEM,
        compiler_params=pltpu.CompilerParams(vmem_limit_bytes=12 << 20),
        name="merge",
    )(base, mine, received)
    one = lax.ppermute(merged[0], "stretch", back(straight))
    two = lax.ppermute(merged[1], "stretch", back(crossed))
    return jnp.concatenate([jnp.where(low, one, two), jnp.where(low, two, one)], axis=1)


def solution(mesh):
    placed = P(("stretch", "seq"), None)
    return jax.shard_map(
        on_device,
        mesh=mesh,
        in_specs=(placed, placed, placed),
        out_specs=placed,
        check_vma=False,
    )
```

```python
import functools
import math

import jax
import jax.numpy as jnp
from jax import lax
from jax.experimental import pallas as pl
from jax.experimental.pallas import tpu as pltpu
from jax.sharding import PartitionSpec as P

QUERY_HEADS = 14
KEY_VALUE_HEADS = 2
HEAD_SIZE = 128
BLOCKS = 4
GROUP = QUERY_HEADS // KEY_VALUE_HEADS
ROWS = 128
STACKED = GROUP * ROWS
X = 4
Y = 8
SPAN = X * ROWS
EXPONENT = math.log2(math.e) / math.sqrt(HEAD_SIZE)
LOWEST = -1e30
CHUNK = 896


def worker(sequence, head, core):
    plane = 4 * (sequence % 2) + 2 * head + 1 - sequence // 2
    return 2 * plane + core


def stretch_pairs(which):
    pairs = []
    for sequence in range(4):
        for block in range(BLOCKS):
            head = (0 if block < 2 else 1) ^ which
            core = 0 if block in (0, 3) else 1
            pairs.append((4 * block + sequence, worker(sequence, head, core)))
    return pairs


def back(pairs):
    return [(b, a) for a, b in pairs]


def plane_shift(dx, dy):
    pairs = []
    for y in range(Y):
        for x in range(X):
            for g in range(16):
                target = ((y + dy) % Y) * X + (x + dx) % X
                pairs.append(((y * X + x) * 16 + g, target * 16 + g))
    return pairs


SWAP = [(i, i ^ 1) for i in range(16)]


def shifted(array, dx, dy):
    return lax.ppermute(array, ("seq", "stretch"), plane_shift(dx, dy))


def tables(positions):
    half = HEAD_SIZE // 2
    lane = jnp.arange(HEAD_SIZE, dtype=jnp.int32)
    inverse = 10000000.0 ** (-((lane % half).astype(jnp.float32) * 2.0) / HEAD_SIZE)
    angles = positions.astype(jnp.float32)[..., None] * inverse
    return jnp.cos(angles), jnp.where(lane < half, -jnp.sin(angles), jnp.sin(angles))


def spin(x, cosine, sine):
    return x * cosine + pltpu.roll(x, HEAD_SIZE // 2, 1) * sine


VMEM = pl.BlockSpec(memory_space=pltpu.VMEM)
SMEM = pl.BlockSpec(memory_space=pltpu.SMEM)


def key_kernel(where_ref, one_ref, two_ref, cosine_ref, sine_ref, out_ref):
    head = where_ref[0]
    cosine = cosine_ref[0]
    sine = sine_ref[0]
    for k, ref in enumerate((one_ref, two_ref)):
        place = pl.multiple_of((head ^ k) * (2 * HEAD_SIZE), 2 * HEAD_SIZE)
        x = ref[:, :HEAD_SIZE].astype(jnp.float32)
        out_ref[:, pl.ds(place, HEAD_SIZE)] = spin(x, cosine, sine).astype(jnp.bfloat16)
        out_ref[:, pl.ds(place + HEAD_SIZE, HEAD_SIZE)] = ref[:, HEAD_SIZE : 2 * HEAD_SIZE]


def query_kernel(where_ref, own_ref, other_ref, cosine_ref, sine_ref, out_ref):
    head = where_ref[0]
    core = where_ref[1]

    def turn(ref, which, kind, slot):
        cosine = cosine_ref[kind]
        sine = sine_ref[kind]
        for g in range(GROUP):
            x = ref[which, :, g * HEAD_SIZE : (g + 1) * HEAD_SIZE].astype(jnp.float32)
            out_ref[slot, g * ROWS : (g + 1) * ROWS, :] = spin(x, cosine, sine).astype(jnp.bfloat16)

    turn(own_ref, head, 0, 0)
    turn(own_ref, 1 - head, 0, 1)
    turn(other_ref, 1 - head, 2, 3)

    @pl.when(core == 0)
    def _():
        turn(other_ref, head, 1, 2)
        turn(own_ref, 1 - head, 2, 4)

    @pl.when(core == 1)
    def _():
        turn(own_ref, 1 - head, 1, 2)
        turn(other_ref, 1 - head, 1, 4)


def lanes(x, count):
    return [x[:, j * HEAD_SIZE : (j + 1) * HEAD_SIZE] for j in range(count)]


def absorb(query_ref, query, pairs, acc_ref, top_ref, sum_ref, slot, limit):
    def score(c):
        part = query_ref[query, c * CHUNK : (c + 1) * CHUNK, :]
        return [
            lax.dot_general(
                part, keys, (((1,), (1,)), ((), ())), preferred_element_type=jnp.float32
            )
            for keys, _ in pairs
        ]

    steps = STACKED // CHUNK
    coming = score(0)
    for c in range(steps):
        scores = coming
        if c + 1 < steps:
            coming = score(c + 1)
        if limit is not None:
            row = lax.broadcasted_iota(jnp.int32, (CHUNK, SPAN), 0) + c * CHUNK
            inside = limit[0] <= (row & (ROWS - 1)) + limit[1]
            scores = [jnp.where(inside, s, LOWEST) for s in scores]
        rows = pl.ds(c * CHUNK, CHUNK)
        parts = [part for s in scores for part in lanes(s, s.shape[1] // HEAD_SIZE)]
        highest = parts[0]
        for j in range(1, len(parts)):
            highest = jnp.maximum(highest, parts[j])
        before = top_ref[slot, rows, :]
        top = jnp.maximum(before, jnp.max(highest, axis=-1, keepdims=True))
        scaled = top * EXPONENT
        weights = [jnp.exp2(part * EXPONENT - scaled) for part in parts]
        fade = jnp.exp2(before * EXPONENT - scaled)
        total = weights[0]
        for j in range(1, len(parts)):
            total = total + weights[j]
        product = None
        used = 0
        for _, values in pairs:
            count = values.shape[0] // HEAD_SIZE
            some = weights[used : used + count]
            used += count
            packed = jnp.concatenate([w.astype(jnp.bfloat16) for w in some], axis=1)
            more = jnp.dot(packed, values, preferred_element_type=jnp.float32)
            product = more if product is None else product + more
        top_ref[slot, rows, :] = top
        sum_ref[slot, rows, :] = sum_ref[slot, rows, :] * fade + total
        acc_ref[slot, rows, :] = acc_ref[slot, rows, :] * fade + product


def attend_kernel(first, last, offsets, where_ref, query_ref, *refs):
    number = 1 if first else len(offsets)
    block_refs = refs[:number]
    refs = refs[number:]
    if last:
        out_refs = refs[3:5]
        refs = refs[:3] + refs[5:]
    if not first:
        for source, target in zip(refs[:3], refs[3:6]):
            target[...] = source[...]
        refs = refs[3:]
    acc_ref, top_ref, sum_ref = refs[:3]
    core = where_ref[1]
    x = where_ref[2]
    y = where_ref[3]
    if first:
        acc_ref[...] = jnp.zeros_like(acc_ref)
        top_ref[...] = jnp.full_like(top_ref, LOWEST)
        sum_ref[...] = jnp.zeros_like(sum_ref)
    run = functools.partial(
        absorb, query_ref, acc_ref=acc_ref, top_ref=top_ref, sum_ref=sum_ref
    )

    def columns(ref, place):
        keys = ref[:, pl.ds(place, HEAD_SIZE)]
        values = ref[:, pl.ds(place + HEAD_SIZE, HEAD_SIZE)]
        return keys, values

    def causal(refs, limit):
        def body(query, carry):
            place = pl.multiple_of(query * (2 * HEAD_SIZE), 2 * HEAD_SIZE)
            run(query=query, pairs=[columns(ref, place) for ref in refs], slot=query, limit=limit)
            return carry

        lax.fori_loop(0, 2, body, 0)

    third = pl.multiple_of(core * (2 * HEAD_SIZE), 2 * HEAD_SIZE)
    pairs = [columns(ref, 0) for ref in block_refs]
    run(query=2, pairs=pairs, slot=2 - core, limit=None)
    run(query=3, pairs=pairs, slot=3, limit=None)
    pairs = [columns(ref, third) for ref in block_refs]
    run(query=4, pairs=pairs, slot=1 + 2 * core, limit=None)
    if first:
        column = lax.broadcasted_iota(jnp.int32, (CHUNK, SPAN), 1)
        causal(block_refs[:1], (column, x * ROWS))
    else:
        for offset in sorted(set(offsets)):

            @pl.when(((y + offset) & (Y - 1)) < y)
            def _(offset=offset):
                causal([block_refs[b] for b in range(number) if offsets[b] == offset], None)

    if last:
        lane = lax.broadcasted_iota(jnp.int32, (STACKED, HEAD_SIZE), 1)
        for k in range(4):
            ref = out_refs[k // 2]
            total = jnp.sum(sum_ref[k], axis=-1, keepdims=True)
            ref[k % 2, :, :HEAD_SIZE] = acc_ref[k]
            ref[k % 2, :, HEAD_SIZE:] = jnp.where(lane < HEAD_SIZE // 2, top_ref[k], total)


def attend(where, query, blocks, offsets, state, first=False, last=False):
    number = len(blocks)
    block = jax.ShapeDtypeStruct((4, STACKED, HEAD_SIZE), jnp.float32)
    outs = [block] * 3
    if last:
        outs = [jax.ShapeDtypeStruct((2, STACKED, 2 * HEAD_SIZE), jnp.float32)] * 2
    flops = number * 4 * 4 * STACKED * SPAN * HEAD_SIZE
    return pl.pallas_call(
        functools.partial(attend_kernel, first, last, offsets),
        out_shape=outs,
        in_specs=[SMEM] + [VMEM] * (1 + number + len(state)),
        out_specs=[VMEM] * len(outs),
        scratch_shapes=[pltpu.VMEM(block.shape, block.dtype)] * 3 if last else [],
        cost_estimate=pl.CostEstimate(
            flops=flops, bytes_accessed=4 << 20, transcendentals=number * 4 * STACKED * SPAN
        ),
        compiler_params=pltpu.CompilerParams(vmem_limit_bytes=24 << 20),
        name="attend",
    )(where, query, *blocks, *state)


def halves(stats):
    lane = lax.broadcasted_iota(jnp.int32, stats.shape, 1)
    turned = pltpu.roll(stats, HEAD_SIZE // 2, 1)
    left = lane < HEAD_SIZE // 2
    return jnp.where(left, stats, turned), jnp.where(left, turned, stats)


def merge_kernel(where_ref, own_ref, other_ref, out_ref):
    head = where_ref[0]
    for k in range(2):
        place = head if k == 0 else 1 - head
        for g in range(GROUP):
            rows = slice(g * ROWS, (g + 1) * ROWS)
            top, own_sum = halves(own_ref[k, rows, HEAD_SIZE:])
            other_top, other_sum = halves(other_ref[k, rows, HEAD_SIZE:])
            highest = jnp.maximum(top, other_top)
            mine = jnp.exp2((top - highest) * EXPONENT)
            theirs = jnp.exp2((other_top - highest) * EXPONENT)
            total = own_sum * mine + other_sum * theirs
            value = own_ref[k, rows, :HEAD_SIZE] * mine + other_ref[k, rows, :HEAD_SIZE] * theirs
            out_ref[place, :, g * HEAD_SIZE : (g + 1) * HEAD_SIZE] = (value / total).astype(
                jnp.bfloat16
            )


def on_device(queries, keys, values):
    seq = lax.axis_index("seq")
    stretch = lax.axis_index("stretch")
    x = seq % X
    y = seq // X
    home_block = stretch // 4
    low = home_block < 2
    core = stretch % 2
    head = (stretch // 4) % 2
    positions = seq * ROWS + jnp.arange(ROWS, dtype=jnp.int32)
    length = ROWS * X * Y
    kind = jnp.arange(3, dtype=jnp.int32)[:, None]
    every = jnp.where(kind == 2, 2 * length - 1, positions[None, :] + kind * length)
    cosine, sine = tables(every)
    base = jnp.stack([head, core, x, y]).astype(jnp.int32)
    straight, crossed = stretch_pairs(0), stretch_pairs(1)

    half = GROUP * HEAD_SIZE

    def halves_of(first, second):
        return jnp.where(low, first, second), jnp.where(low, second, first)

    def spread(first, second):
        one = lax.ppermute(first, "stretch", straight)
        two = lax.ppermute(second, "stretch", crossed)
        return one, two

    packs = [
        jnp.concatenate([keys[:, k : k + HEAD_SIZE], values[:, k : k + HEAD_SIZE]], axis=1)
        for k in (0, HEAD_SIZE)
    ]
    one, two = spread(*halves_of(*packs))
    own = pl.pallas_call(
        key_kernel,
        out_shape=jax.ShapeDtypeStruct((ROWS, 4 * HEAD_SIZE), jnp.bfloat16),
        in_specs=[SMEM] + [VMEM] * 4,
        out_specs=VMEM,
        compiler_params=pltpu.CompilerParams(vmem_limit_bytes=8 << 20),
        name="turn_keys",
    )(base, one, two, cosine, sine)
    lines = [[X * line + k for k in range(X)] for line in range(Y)]
    row = lax.all_gather(own, "seq", axis=0, tiled=True, axis_index_groups=lines)
    straight_half, crossed_half = halves_of(queries[:, :half], queries[:, half:])
    row, crossed_half = lax.optimization_barrier((row, crossed_half))
    raw = jnp.stack(spread(straight_half, crossed_half))
    other_raw = lax.ppermute(raw, "stretch", SWAP)
    query = pl.pallas_call(
        query_kernel,
        out_shape=jax.ShapeDtypeStruct((5, STACKED, HEAD_SIZE), jnp.bfloat16),
        in_specs=[SMEM] + [VMEM] * 4,
        out_specs=VMEM,
        cost_estimate=pl.CostEstimate(flops=2 << 30, bytes_accessed=4 << 20, transcendentals=0),
        compiler_params=pltpu.CompilerParams(vmem_limit_bytes=12 << 20),
        name="turn_queries",
    )(base, raw, other_raw, cosine, sine)
    rounds = [(row,)]
    states = []

    def step(hop, ahead):
        up, down = rounds[-1][0], rounds[-1][-1]
        if hop == Y // 2:
            up, down = up[: SPAN // 2], down[SPAN // 2 :]
        if ahead is not None:
            up, _ = lax.optimization_barrier((up, ahead))
            down, _ = lax.optimization_barrier((down, ahead))
        rounds.append((shifted(up, 0, 1), shifted(down, 0, -1)))

    step(1, None)
    step(2, None)
    for hop in range(Y // 2):
        states.append(
            attend(
                base, query, rounds[hop], (-hop, hop), states[-1] if states else [], first=hop == 0
            )
        )
        if hop < 2:
            step(hop + 3, states[-1][2])
    mine, send = attend(base, query, rounds[4], (4, 4), states[-1], last=True)
    received = lax.ppermute(send, "stretch", SWAP)
    merged = pl.pallas_call(
        merge_kernel,
        out_shape=jax.ShapeDtypeStruct((2, ROWS, half), jnp.bfloat16),
        in_specs=[SMEM] + [VMEM] * 2,
        out_specs=VMEM,
        compiler_params=pltpu.CompilerParams(vmem_limit_bytes=12 << 20),
        name="merge",
    )(base, mine, received)
    one = lax.ppermute(merged[0], "stretch", back(straight))
    two = lax.ppermute(merged[1], "stretch", back(crossed))
    return jnp.concatenate([jnp.where(low, one, two), jnp.where(low, two, one)], axis=1)


def solution(mesh):
    placed = P(("stretch", "seq"), None)
    return jax.shard_map(
        on_device,
        mesh=mesh,
        in_specs=(placed, placed, placed),
        out_specs=placed,
        check_vma=False,
    )
```

```python
import functools
import math

import jax
import jax.numpy as jnp
from jax import lax
from jax.experimental import pallas as pl
from jax.experimental.pallas import tpu as pltpu
from jax.sharding import PartitionSpec as P

QUERY_HEADS = 14
KEY_VALUE_HEADS = 2
HEAD_SIZE = 128
BLOCKS = 4
GROUP = QUERY_HEADS // KEY_VALUE_HEADS
ROWS = 128
STACKED = GROUP * ROWS
X = 4
Y = 8
SPAN = X * ROWS
EXPONENT = math.log2(math.e) / math.sqrt(HEAD_SIZE)
LOWEST = -1e30
CHUNK = 896


def worker(sequence, head, core):
    plane = 4 * (sequence % 2) + 2 * head + 1 - sequence // 2
    return 2 * plane + core


def stretch_pairs(which):
    pairs = []
    for sequence in range(4):
        for block in range(BLOCKS):
            head = (0 if block < 2 else 1) ^ which
            core = 0 if block in (0, 3) else 1
            pairs.append((4 * block + sequence, worker(sequence, head, core)))
    return pairs


def back(pairs):
    return [(b, a) for a, b in pairs]


def plane_shift(dx, dy):
    pairs = []
    for y in range(Y):
        for x in range(X):
            for g in range(16):
                target = ((y + dy) % Y) * X + (x + dx) % X
                pairs.append(((y * X + x) * 16 + g, target * 16 + g))
    return pairs


SWAP = [(i, i ^ 1) for i in range(16)]


def shifted(array, dx, dy):
    return lax.ppermute(array, ("seq", "stretch"), plane_shift(dx, dy))


def tables(positions):
    half = HEAD_SIZE // 2
    lane = jnp.arange(HEAD_SIZE, dtype=jnp.int32)
    inverse = 10000000.0 ** (-((lane % half).astype(jnp.float32) * 2.0) / HEAD_SIZE)
    angles = positions.astype(jnp.float32)[..., None] * inverse
    return jnp.cos(angles), jnp.where(lane < half, -jnp.sin(angles), jnp.sin(angles))


def spin(x, cosine, sine):
    return x * cosine + pltpu.roll(x, HEAD_SIZE // 2, 1) * sine


VMEM = pl.BlockSpec(memory_space=pltpu.VMEM)
SMEM = pl.BlockSpec(memory_space=pltpu.SMEM)


def key_kernel(where_ref, one_ref, two_ref, cosine_ref, sine_ref, out_ref):
    head = where_ref[0]
    cosine = cosine_ref[0]
    sine = sine_ref[0]
    for k, ref in enumerate((one_ref, two_ref)):
        place = pl.multiple_of((head ^ k) * (2 * HEAD_SIZE), 2 * HEAD_SIZE)
        x = ref[:, :HEAD_SIZE].astype(jnp.float32)
        out_ref[:, pl.ds(place, HEAD_SIZE)] = spin(x, cosine, sine).astype(jnp.bfloat16)
        out_ref[:, pl.ds(place + HEAD_SIZE, HEAD_SIZE)] = ref[:, HEAD_SIZE : 2 * HEAD_SIZE]


def query_kernel(where_ref, own_ref, other_ref, cosine_ref, sine_ref, out_ref):
    head = where_ref[0]
    core = where_ref[1]

    def turn(ref, which, kind, slot):
        cosine = cosine_ref[kind]
        sine = sine_ref[kind]
        for g in range(GROUP):
            x = ref[which, :, g * HEAD_SIZE : (g + 1) * HEAD_SIZE].astype(jnp.float32)
            out_ref[slot, g * ROWS : (g + 1) * ROWS, :] = spin(x, cosine, sine).astype(jnp.bfloat16)

    turn(own_ref, head, 0, 0)
    turn(own_ref, 1 - head, 0, 1)
    turn(other_ref, 1 - head, 2, 3)

    @pl.when(core == 0)
    def _():
        turn(other_ref, head, 1, 2)
        turn(own_ref, 1 - head, 2, 4)

    @pl.when(core == 1)
    def _():
        turn(own_ref, 1 - head, 1, 2)
        turn(other_ref, 1 - head, 1, 4)


def lanes(x, count):
    return [x[:, j * HEAD_SIZE : (j + 1) * HEAD_SIZE] for j in range(count)]


def absorb(query_ref, query, pairs, acc_ref, top_ref, sum_ref, slot, limit):
    def score(c):
        part = query_ref[query, c * CHUNK : (c + 1) * CHUNK, :]
        return [
            lax.dot_general(
                part, keys, (((1,), (1,)), ((), ())), preferred_element_type=jnp.float32
            )
            for keys, _ in pairs
        ]

    steps = STACKED // CHUNK
    coming = score(0)
    for c in range(steps):
        scores = coming
        if c + 1 < steps:
            coming = score(c + 1)
        if limit is not None:
            row = lax.broadcasted_iota(jnp.int32, (CHUNK, SPAN), 0) + c * CHUNK
            inside = limit[0] <= (row & (ROWS - 1)) + limit[1]
            scores = [jnp.where(inside, s, LOWEST) for s in scores]
        rows = pl.ds(c * CHUNK, CHUNK)
        parts = [part for s in scores for part in lanes(s, s.shape[1] // HEAD_SIZE)]
        highest = parts[0]
        for j in range(1, len(parts)):
            highest = jnp.maximum(highest, parts[j])
        before = top_ref[slot, rows, :]
        top = jnp.maximum(before, jnp.max(highest, axis=-1, keepdims=True))
        scaled = top * EXPONENT
        weights = [jnp.exp2(part * EXPONENT - scaled) for part in parts]
        fade = jnp.exp2(before * EXPONENT - scaled)
        total = weights[0]
        for j in range(1, len(parts)):
            total = total + weights[j]
        product = None
        used = 0
        for _, values in pairs:
            count = values.shape[0] // HEAD_SIZE
            some = weights[used : used + count]
            used += count
            packed = jnp.concatenate([w.astype(jnp.bfloat16) for w in some], axis=1)
            more = jnp.dot(packed, values, preferred_element_type=jnp.float32)
            product = more if product is None else product + more
        top_ref[slot, rows, :] = top
        sum_ref[slot, rows, :] = sum_ref[slot, rows, :] * fade + total
        acc_ref[slot, rows, :] = acc_ref[slot, rows, :] * fade + product


def attend_kernel(first, last, diagonal, offsets, where_ref, query_ref, *refs):
    number = 1 if first else len(offsets)
    block_refs = refs[:number]
    refs = refs[number:]
    if last:
        send_ref = refs[6]
        own_refs = refs[3:6]
        refs = refs[:3] + refs[7:]
    if not first:
        for source, target in zip(refs[:3], refs[3:6]):
            target[...] = source[...]
        refs = refs[3:]
    acc_ref, top_ref, sum_ref = refs[:3]
    core = where_ref[1]
    x = where_ref[2]
    y = where_ref[3]
    if first:
        acc_ref[...] = jnp.zeros_like(acc_ref)
        top_ref[...] = jnp.full_like(top_ref, LOWEST)
        sum_ref[...] = jnp.zeros_like(sum_ref)
    run = functools.partial(
        absorb, query_ref, acc_ref=acc_ref, top_ref=top_ref, sum_ref=sum_ref
    )

    def columns(ref, place):
        keys = ref[:, pl.ds(place, HEAD_SIZE)]
        values = ref[:, pl.ds(place + HEAD_SIZE, HEAD_SIZE)]
        return keys, values

    def causal(refs, limit):
        def body(query, carry):
            place = pl.multiple_of(query * (2 * HEAD_SIZE), 2 * HEAD_SIZE)
            run(query=query, pairs=[columns(ref, place) for ref in refs], slot=query, limit=limit)
            return carry

        lax.fori_loop(0, 2, body, 0)

    third = pl.multiple_of(core * (2 * HEAD_SIZE), 2 * HEAD_SIZE)
    pairs = [columns(ref, 0) for ref in block_refs]
    run(query=2, pairs=pairs, slot=2 - core, limit=None)
    run(query=3, pairs=pairs, slot=3, limit=None)
    pairs = [columns(ref, third) for ref in block_refs]
    run(query=4, pairs=pairs, slot=1 + 2 * core, limit=None)
    if first:
        column = lax.broadcasted_iota(jnp.int32, (CHUNK, SPAN), 1)
        causal(block_refs[:1], (column, x * ROWS))
    elif diagonal:
        for offset in sorted(set(offsets)):

            @pl.when(((y + offset) & (Y - 1)) < y)
            def _(offset=offset):
                causal([block_refs[b] for b in range(number) if offsets[b] == offset], None)

    if last:
        for state, own in zip((acc_ref, top_ref, sum_ref), own_refs):
            own[...] = state[:2]
        pack(acc_ref, top_ref, sum_ref, 2, send_ref)


def pack(acc_ref, top_ref, sum_ref, start, out_ref):
    lane = lax.broadcasted_iota(jnp.int32, (STACKED, HEAD_SIZE), 1)
    for k in range(2):
        total = jnp.sum(sum_ref[start + k], axis=-1, keepdims=True)
        out_ref[k, :, :HEAD_SIZE] = acc_ref[start + k]
        out_ref[k, :, HEAD_SIZE:] = jnp.where(lane < HEAD_SIZE // 2, top_ref[start + k], total)


def rest_kernel(groups, where_ref, query_ref, *refs):
    y = where_ref[3]
    count = sum(number for _, number in groups)
    block_refs = refs[:count]
    sources = refs[count : count + 3]
    out_ref = refs[count + 3]
    states = refs[count + 4 :]
    for source, target in zip(sources, states):
        target[...] = source[...]
    acc_ref, top_ref, sum_ref = states
    start = 0
    for offset, number in groups:
        members = block_refs[start : start + number]
        start += number

        @pl.when(((y + offset) & (Y - 1)) < y)
        def _(members=members):
            def body(query, carry):
                keys = pl.multiple_of(query * (2 * HEAD_SIZE), 2 * HEAD_SIZE)
                values = pl.multiple_of(keys + HEAD_SIZE, HEAD_SIZE)
                pairs = [
                    (ref[:, pl.ds(keys, HEAD_SIZE)], ref[:, pl.ds(values, HEAD_SIZE)])
                    for ref in members
                ]
                absorb(query_ref, query, pairs, acc_ref, top_ref, sum_ref, query, None)
                return carry

            lax.fori_loop(0, 2, body, 0)

    pack(acc_ref, top_ref, sum_ref, 0, out_ref)


def rest(where, query, blocks, groups, state):
    block = jax.ShapeDtypeStruct((2, STACKED, HEAD_SIZE), jnp.float32)
    return pl.pallas_call(
        functools.partial(rest_kernel, groups),
        out_shape=jax.ShapeDtypeStruct((2, STACKED, 2 * HEAD_SIZE), jnp.float32),
        in_specs=[SMEM] + [VMEM] * (1 + len(blocks) + 3),
        out_specs=VMEM,
        scratch_shapes=[pltpu.VMEM(block.shape, block.dtype)] * 3,
        cost_estimate=pl.CostEstimate(
            flops=12 * STACKED * SPAN * HEAD_SIZE, bytes_accessed=4 << 20, transcendentals=0
        ),
        compiler_params=pltpu.CompilerParams(vmem_limit_bytes=20 << 20),
        name="rest",
    )(where, query, *blocks, *state)


def attend(where, query, blocks, offsets, state, first=False, last=False, diagonal=True):
    number = len(blocks)
    block = jax.ShapeDtypeStruct((4, STACKED, HEAD_SIZE), jnp.float32)
    outs = [block] * 3
    if last:
        outs = [jax.ShapeDtypeStruct((2, STACKED, HEAD_SIZE), jnp.float32)] * 3
        outs.append(jax.ShapeDtypeStruct((2, STACKED, 2 * HEAD_SIZE), jnp.float32))
    flops = number * 4 * 4 * STACKED * SPAN * HEAD_SIZE
    return pl.pallas_call(
        functools.partial(attend_kernel, first, last, diagonal, offsets),
        out_shape=outs,
        in_specs=[SMEM] + [VMEM] * (1 + number + len(state)),
        out_specs=[VMEM] * len(outs),
        scratch_shapes=[pltpu.VMEM(block.shape, block.dtype)] * 3 if last else [],
        cost_estimate=pl.CostEstimate(
            flops=flops, bytes_accessed=4 << 20, transcendentals=number * 4 * STACKED * SPAN
        ),
        compiler_params=pltpu.CompilerParams(vmem_limit_bytes=24 << 20),
        name="attend",
    )(where, query, *blocks, *state)


def halves(stats):
    lane = lax.broadcasted_iota(jnp.int32, stats.shape, 1)
    turned = pltpu.roll(stats, HEAD_SIZE // 2, 1)
    left = lane < HEAD_SIZE // 2
    return jnp.where(left, stats, turned), jnp.where(left, turned, stats)


def merge_kernel(where_ref, own_ref, other_ref, out_ref):
    head = where_ref[0]
    for k in range(2):
        place = head if k == 0 else 1 - head
        for g in range(GROUP):
            rows = slice(g * ROWS, (g + 1) * ROWS)
            top, own_sum = halves(own_ref[k, rows, HEAD_SIZE:])
            other_top, other_sum = halves(other_ref[k, rows, HEAD_SIZE:])
            highest = jnp.maximum(top, other_top)
            mine = jnp.exp2((top - highest) * EXPONENT)
            theirs = jnp.exp2((other_top - highest) * EXPONENT)
            total = own_sum * mine + other_sum * theirs
            value = own_ref[k, rows, :HEAD_SIZE] * mine + other_ref[k, rows, :HEAD_SIZE] * theirs
            out_ref[place, :, g * HEAD_SIZE : (g + 1) * HEAD_SIZE] = (value / total).astype(
                jnp.bfloat16
            )


def on_device(queries, keys, values):
    seq = lax.axis_index("seq")
    stretch = lax.axis_index("stretch")
    x = seq % X
    y = seq // X
    home_block = stretch // 4
    low = home_block < 2
    core = stretch % 2
    head = (stretch // 4) % 2
    positions = seq * ROWS + jnp.arange(ROWS, dtype=jnp.int32)
    length = ROWS * X * Y
    kind = jnp.arange(3, dtype=jnp.int32)[:, None]
    every = jnp.where(kind == 2, 2 * length - 1, positions[None, :] + kind * length)
    cosine, sine = tables(every)
    base = jnp.stack([head, core, x, y]).astype(jnp.int32)
    straight, crossed = stretch_pairs(0), stretch_pairs(1)

    half = GROUP * HEAD_SIZE

    def halves_of(first, second):
        return jnp.where(low, first, second), jnp.where(low, second, first)

    def spread(first, second):
        one = lax.ppermute(first, "stretch", straight)
        two = lax.ppermute(second, "stretch", crossed)
        return one, two

    packs = [
        jnp.concatenate([keys[:, k : k + HEAD_SIZE], values[:, k : k + HEAD_SIZE]], axis=1)
        for k in (0, HEAD_SIZE)
    ]
    one, two = spread(*halves_of(*packs))
    own = pl.pallas_call(
        key_kernel,
        out_shape=jax.ShapeDtypeStruct((ROWS, 4 * HEAD_SIZE), jnp.bfloat16),
        in_specs=[SMEM] + [VMEM] * 4,
        out_specs=VMEM,
        compiler_params=pltpu.CompilerParams(vmem_limit_bytes=8 << 20),
        name="turn_keys",
    )(base, one, two, cosine, sine)
    lines = [[X * line + k for k in range(X)] for line in range(Y)]
    row = lax.all_gather(own, "seq", axis=0, tiled=True, axis_index_groups=lines)
    straight_half, crossed_half = halves_of(queries[:, :half], queries[:, half:])
    row, crossed_half = lax.optimization_barrier((row, crossed_half))
    raw = jnp.stack(spread(straight_half, crossed_half))
    other_raw = lax.ppermute(raw, "stretch", SWAP)
    query = pl.pallas_call(
        query_kernel,
        out_shape=jax.ShapeDtypeStruct((5, STACKED, HEAD_SIZE), jnp.bfloat16),
        in_specs=[SMEM] + [VMEM] * 4,
        out_specs=VMEM,
        cost_estimate=pl.CostEstimate(flops=2 << 30, bytes_accessed=4 << 20, transcendentals=0),
        compiler_params=pltpu.CompilerParams(vmem_limit_bytes=12 << 20),
        name="turn_queries",
    )(base, raw, other_raw, cosine, sine)
    rounds = [(row,)]
    states = []

    def step(hop, ahead):
        up, down = rounds[-1][0], rounds[-1][-1]
        if hop == Y // 2:
            up, down = up[: SPAN // 2], down[SPAN // 2 :]
        if ahead is not None:
            up, _ = lax.optimization_barrier((up, ahead))
            down, _ = lax.optimization_barrier((down, ahead))
        rounds.append((shifted(up, 0, 1), shifted(down, 0, -1)))

    step(1, None)
    step(2, None)
    for hop in range(Y // 2):
        before = states[-1] if states else []
        states.append(
            attend(
                base,
                query,
                rounds[hop],
                (-hop, hop),
                before,
                first=hop == 0,
                diagonal=hop < 3,
            )
        )
        if hop in (1, 2):
            step(hop + 2, states[-1][2])
    *kept, send = attend(base, query, rounds[4], (4, 4), states[-1], last=True, diagonal=False)
    received = lax.ppermute(send, "stretch", SWAP)
    mine = rest(base, query, [*rounds[3], *rounds[4]], ((-3, 1), (3, 1), (4, 2)), kept)
    merged = pl.pallas_call(
        merge_kernel,
        out_shape=jax.ShapeDtypeStruct((2, ROWS, half), jnp.bfloat16),
        in_specs=[SMEM] + [VMEM] * 2,
        out_specs=VMEM,
        compiler_params=pltpu.CompilerParams(vmem_limit_bytes=12 << 20),
        name="merge",
    )(base, mine, received)
    one = lax.ppermute(merged[0], "stretch", back(straight))
    two = lax.ppermute(merged[1], "stretch", back(crossed))
    return jnp.concatenate([jnp.where(low, one, two), jnp.where(low, two, one)], axis=1)


def solution(mesh):
    placed = P(("stretch", "seq"), None)
    return jax.shard_map(
        on_device,
        mesh=mesh,
        in_specs=(placed, placed, placed),
        out_specs=placed,
        check_vma=False,
    )
```

```python
import functools
import math

import jax
import jax.numpy as jnp
from jax import lax
from jax.experimental import pallas as pl
from jax.experimental.pallas import tpu as pltpu
from jax.sharding import PartitionSpec as P

QUERY_HEADS = 14
KEY_VALUE_HEADS = 2
HEAD_SIZE = 128
BLOCKS = 4
GROUP = QUERY_HEADS // KEY_VALUE_HEADS
ROWS = 128
STACKED = GROUP * ROWS
X = 4
Y = 8
SPAN = X * ROWS
EXPONENT = math.log2(math.e) / math.sqrt(HEAD_SIZE)
LOWEST = -1e30
CHUNK = 896


def worker(sequence, head, core):
    plane = 4 * (sequence % 2) + 2 * head + 1 - sequence // 2
    return 2 * plane + core


def stretch_pairs(which):
    pairs = []
    for sequence in range(4):
        for block in range(BLOCKS):
            head = (0 if block < 2 else 1) ^ which
            core = 0 if block in (0, 3) else 1
            pairs.append((4 * block + sequence, worker(sequence, head, core)))
    return pairs


def back(pairs):
    return [(b, a) for a, b in pairs]


def plane_shift(dx, dy):
    pairs = []
    for y in range(Y):
        for x in range(X):
            for g in range(16):
                target = ((y + dy) % Y) * X + (x + dx) % X
                pairs.append(((y * X + x) * 16 + g, target * 16 + g))
    return pairs


SWAP = [(i, i ^ 1) for i in range(16)]


def shifted(array, dx, dy):
    return lax.ppermute(array, ("seq", "stretch"), plane_shift(dx, dy))


def tables(positions):
    half = HEAD_SIZE // 2
    lane = jnp.arange(HEAD_SIZE, dtype=jnp.int32)
    inverse = 10000000.0 ** (-((lane % half).astype(jnp.float32) * 2.0) / HEAD_SIZE)
    angles = positions.astype(jnp.float32)[..., None] * inverse
    return jnp.cos(angles), jnp.where(lane < half, -jnp.sin(angles), jnp.sin(angles))


def spin(x, cosine, sine):
    return x * cosine + pltpu.roll(x, HEAD_SIZE // 2, 1) * sine


VMEM = pl.BlockSpec(memory_space=pltpu.VMEM)
SMEM = pl.BlockSpec(memory_space=pltpu.SMEM)


def key_kernel(where_ref, one_ref, two_ref, cosine_ref, sine_ref, out_ref):
    head = where_ref[0]
    cosine = cosine_ref[0]
    sine = sine_ref[0]
    for k, ref in enumerate((one_ref, two_ref)):
        place = pl.multiple_of((head ^ k) * (2 * HEAD_SIZE), 2 * HEAD_SIZE)
        x = ref[:, :HEAD_SIZE].astype(jnp.float32)
        out_ref[:, pl.ds(place, HEAD_SIZE)] = spin(x, cosine, sine).astype(jnp.bfloat16)
        out_ref[:, pl.ds(place + HEAD_SIZE, HEAD_SIZE)] = ref[:, HEAD_SIZE : 2 * HEAD_SIZE]


def query_kernel(where_ref, own_ref, other_ref, cosine_ref, sine_ref, out_ref):
    head = where_ref[0]
    core = where_ref[1]

    def turn(ref, which, kind, slot):
        cosine = cosine_ref[kind]
        sine = sine_ref[kind]
        for g in range(GROUP):
            x = ref[which, :, g * HEAD_SIZE : (g + 1) * HEAD_SIZE].astype(jnp.float32)
            out_ref[slot, g * ROWS : (g + 1) * ROWS, :] = spin(x, cosine, sine).astype(jnp.bfloat16)

    turn(own_ref, head, 0, 0)
    turn(own_ref, 1 - head, 0, 1)
    turn(other_ref, 1 - head, 2, 3)

    @pl.when(core == 0)
    def _():
        turn(other_ref, head, 1, 2)
        turn(own_ref, 1 - head, 2, 4)

    @pl.when(core == 1)
    def _():
        turn(own_ref, 1 - head, 1, 2)
        turn(other_ref, 1 - head, 1, 4)


def lanes(x, count):
    return [x[:, j * HEAD_SIZE : (j + 1) * HEAD_SIZE] for j in range(count)]


def absorb(query_ref, query, pairs, acc_ref, top_ref, sum_ref, slot, limit):
    def score(c):
        part = query_ref[query, c * CHUNK : (c + 1) * CHUNK, :]
        return [
            lax.dot_general(
                part, keys, (((1,), (1,)), ((), ())), preferred_element_type=jnp.float32
            )
            for keys, _ in pairs
        ]

    steps = STACKED // CHUNK
    coming = score(0)
    for c in range(steps):
        scores = coming
        if c + 1 < steps:
            coming = score(c + 1)
        if limit is not None:
            row = lax.broadcasted_iota(jnp.int32, (CHUNK, SPAN), 0) + c * CHUNK
            inside = limit[0] <= (row & (ROWS - 1)) + limit[1]
            scores = [jnp.where(inside, s, LOWEST) for s in scores]
        rows = pl.ds(c * CHUNK, CHUNK)
        parts = [part for s in scores for part in lanes(s, s.shape[1] // HEAD_SIZE)]
        highest = parts[0]
        for j in range(1, len(parts)):
            highest = jnp.maximum(highest, parts[j])
        before = top_ref[slot, rows, :]
        top = jnp.maximum(before, jnp.max(highest, axis=-1, keepdims=True))
        scaled = top * EXPONENT
        weights = [jnp.exp2(part * EXPONENT - scaled) for part in parts]
        fade = jnp.exp2(before * EXPONENT - scaled)
        total = weights[0]
        for j in range(1, len(parts)):
            total = total + weights[j]
        product = None
        used = 0
        for _, values in pairs:
            count = values.shape[0] // HEAD_SIZE
            some = weights[used : used + count]
            used += count
            packed = jnp.concatenate([w.astype(jnp.bfloat16) for w in some], axis=1)
            more = jnp.dot(packed, values, preferred_element_type=jnp.float32)
            product = more if product is None else product + more
        top_ref[slot, rows, :] = top
        sum_ref[slot, rows, :] = sum_ref[slot, rows, :] * fade + total
        acc_ref[slot, rows, :] = acc_ref[slot, rows, :] * fade + product


def attend_kernel(first, last, diagonal, offsets, where_ref, query_ref, *refs):
    number = 1 if first else len(offsets)
    block_refs = refs[:number]
    refs = refs[number:]
    if last:
        send_ref = refs[6]
        own_refs = refs[3:6]
        refs = refs[:3] + refs[7:]
    if not first:
        for source, target in zip(refs[:3], refs[3:6]):
            target[...] = source[...]
        refs = refs[3:]
    acc_ref, top_ref, sum_ref = refs[:3]
    core = where_ref[1]
    x = where_ref[2]
    y = where_ref[3]
    if first:
        acc_ref[...] = jnp.zeros_like(acc_ref)
        top_ref[...] = jnp.full_like(top_ref, LOWEST)
        sum_ref[...] = jnp.zeros_like(sum_ref)
    run = functools.partial(
        absorb, query_ref, acc_ref=acc_ref, top_ref=top_ref, sum_ref=sum_ref
    )

    def columns(ref, place):
        keys = ref[:, pl.ds(place, HEAD_SIZE)]
        values = ref[:, pl.ds(place + HEAD_SIZE, HEAD_SIZE)]
        return keys, values

    def causal(refs, limit):
        def body(query, carry):
            place = pl.multiple_of(query * (2 * HEAD_SIZE), 2 * HEAD_SIZE)
            run(query=query, pairs=[columns(ref, place) for ref in refs], slot=query, limit=limit)
            return carry

        lax.fori_loop(0, 2, body, 0)

    third = pl.multiple_of(core * (2 * HEAD_SIZE), 2 * HEAD_SIZE)
    pairs = [columns(ref, 0) for ref in block_refs]
    run(query=2, pairs=pairs, slot=2 - core, limit=None)
    run(query=3, pairs=pairs, slot=3, limit=None)
    pairs = [columns(ref, third) for ref in block_refs]
    run(query=4, pairs=pairs, slot=1 + 2 * core, limit=None)
    if first:
        column = lax.broadcasted_iota(jnp.int32, (CHUNK, SPAN), 1)
        causal(block_refs[:1], (column, x * ROWS))
    elif diagonal:
        for offset in sorted(set(offsets)):

            @pl.when(((y + offset) & (Y - 1)) < y)
            def _(offset=offset):
                causal([block_refs[b] for b in range(number) if offsets[b] == offset], None)

    if last:
        for state, own in zip((acc_ref, top_ref, sum_ref), own_refs):
            own[...] = state[:2]
        pack(acc_ref, top_ref, sum_ref, 2, send_ref)


def pack(acc_ref, top_ref, sum_ref, start, out_ref):
    lane = lax.broadcasted_iota(jnp.int32, (STACKED, HEAD_SIZE), 1)
    for k in range(2):
        total = jnp.sum(sum_ref[start + k], axis=-1, keepdims=True)
        out_ref[k, :, :HEAD_SIZE] = acc_ref[start + k]
        out_ref[k, :, HEAD_SIZE:] = jnp.where(lane < HEAD_SIZE // 2, top_ref[start + k], total)


def rest_kernel(groups, where_ref, query_ref, *refs):
    y = where_ref[3]
    count = sum(number for _, number in groups)
    block_refs = refs[:count]
    sources = refs[count : count + 3]
    out_ref = refs[count + 3]
    states = refs[count + 4 :]
    for source, target in zip(sources, states):
        target[...] = source[...]
    acc_ref, top_ref, sum_ref = states
    start = 0
    for offset, number in groups:
        members = block_refs[start : start + number]
        start += number

        @pl.when(((y + offset) & (Y - 1)) < y)
        def _(members=members):
            def body(query, carry):
                keys = pl.multiple_of(query * (2 * HEAD_SIZE), 2 * HEAD_SIZE)
                values = pl.multiple_of(keys + HEAD_SIZE, HEAD_SIZE)
                pairs = [
                    (ref[:, pl.ds(keys, HEAD_SIZE)], ref[:, pl.ds(values, HEAD_SIZE)])
                    for ref in members
                ]
                absorb(query_ref, query, pairs, acc_ref, top_ref, sum_ref, query, None)
                return carry

            lax.fori_loop(0, 2, body, 0)

    pack(acc_ref, top_ref, sum_ref, 0, out_ref)


def rest(where, query, blocks, groups, state):
    block = jax.ShapeDtypeStruct((2, STACKED, HEAD_SIZE), jnp.float32)
    return pl.pallas_call(
        functools.partial(rest_kernel, groups),
        out_shape=jax.ShapeDtypeStruct((2, STACKED, 2 * HEAD_SIZE), jnp.float32),
        in_specs=[SMEM] + [VMEM] * (1 + len(blocks) + 3),
        out_specs=VMEM,
        scratch_shapes=[pltpu.VMEM(block.shape, block.dtype)] * 3,
        cost_estimate=pl.CostEstimate(
            flops=12 * STACKED * SPAN * HEAD_SIZE, bytes_accessed=4 << 20, transcendentals=0
        ),
        compiler_params=pltpu.CompilerParams(vmem_limit_bytes=20 << 20),
        name="rest",
    )(where, query, *blocks, *state)


def attend(where, query, blocks, offsets, state, first=False, last=False, diagonal=True):
    number = len(blocks)
    block = jax.ShapeDtypeStruct((4, STACKED, HEAD_SIZE), jnp.float32)
    outs = [block] * 3
    if last:
        outs = [jax.ShapeDtypeStruct((2, STACKED, HEAD_SIZE), jnp.float32)] * 3
        outs.append(jax.ShapeDtypeStruct((2, STACKED, 2 * HEAD_SIZE), jnp.float32))
    flops = number * 4 * 4 * STACKED * SPAN * HEAD_SIZE
    return pl.pallas_call(
        functools.partial(attend_kernel, first, last, diagonal, offsets),
        out_shape=outs,
        in_specs=[SMEM] + [VMEM] * (1 + number + len(state)),
        out_specs=[VMEM] * len(outs),
        scratch_shapes=[pltpu.VMEM(block.shape, block.dtype)] * 3 if last else [],
        cost_estimate=pl.CostEstimate(
            flops=flops, bytes_accessed=4 << 20, transcendentals=number * 4 * STACKED * SPAN
        ),
        compiler_params=pltpu.CompilerParams(vmem_limit_bytes=24 << 20),
        name="attend",
    )(where, query, *blocks, *state)


def halves(stats):
    lane = lax.broadcasted_iota(jnp.int32, stats.shape, 1)
    turned = pltpu.roll(stats, HEAD_SIZE // 2, 1)
    left = lane < HEAD_SIZE // 2
    return jnp.where(left, stats, turned), jnp.where(left, turned, stats)


def merge_kernel(where_ref, own_ref, other_ref, out_ref):
    head = where_ref[0]
    for k in range(2):
        place = head if k == 0 else 1 - head
        for g in range(GROUP):
            rows = slice(g * ROWS, (g + 1) * ROWS)
            top, own_sum = halves(own_ref[k, rows, HEAD_SIZE:])
            other_top, other_sum = halves(other_ref[k, rows, HEAD_SIZE:])
            highest = jnp.maximum(top, other_top)
            mine = jnp.exp2((top - highest) * EXPONENT)
            theirs = jnp.exp2((other_top - highest) * EXPONENT)
            total = own_sum * mine + other_sum * theirs
            value = own_ref[k, rows, :HEAD_SIZE] * mine + other_ref[k, rows, :HEAD_SIZE] * theirs
            out_ref[place, :, g * HEAD_SIZE : (g + 1) * HEAD_SIZE] = (value / total).astype(
                jnp.bfloat16
            )


def on_device(queries, keys, values):
    seq = lax.axis_index("seq")
    stretch = lax.axis_index("stretch")
    x = seq % X
    y = seq // X
    home_block = stretch // 4
    low = home_block < 2
    core = stretch % 2
    head = (stretch // 4) % 2
    positions = seq * ROWS + jnp.arange(ROWS, dtype=jnp.int32)
    length = ROWS * X * Y
    kind = jnp.arange(3, dtype=jnp.int32)[:, None]
    every = jnp.where(kind == 2, 2 * length - 1, positions[None, :] + kind * length)
    cosine, sine = tables(every)
    base = jnp.stack([head, core, x, y]).astype(jnp.int32)
    straight, crossed = stretch_pairs(0), stretch_pairs(1)

    half = GROUP * HEAD_SIZE

    def halves_of(first, second):
        return jnp.where(low, first, second), jnp.where(low, second, first)

    def spread(first, second):
        one = lax.ppermute(first, "stretch", straight)
        two = lax.ppermute(second, "stretch", crossed)
        return one, two

    packs = [
        jnp.concatenate([keys[:, k : k + HEAD_SIZE], values[:, k : k + HEAD_SIZE]], axis=1)
        for k in (0, HEAD_SIZE)
    ]
    one, two = spread(*halves_of(*packs))
    own = pl.pallas_call(
        key_kernel,
        out_shape=jax.ShapeDtypeStruct((ROWS, 4 * HEAD_SIZE), jnp.bfloat16),
        in_specs=[SMEM] + [VMEM] * 4,
        out_specs=VMEM,
        compiler_params=pltpu.CompilerParams(vmem_limit_bytes=8 << 20),
        name="turn_keys",
    )(base, one, two, cosine, sine)
    lines = [[X * line + k for k in range(X)] for line in range(Y)]
    row = lax.all_gather(own, "seq", axis=0, tiled=True, axis_index_groups=lines)
    straight_half, crossed_half = halves_of(queries[:, :half], queries[:, half:])
    row, *arrived = lax.optimization_barrier((row, *spread(straight_half, crossed_half)))
    raw = jnp.stack(arrived)
    other_raw = lax.ppermute(raw, "stretch", SWAP)
    query = pl.pallas_call(
        query_kernel,
        out_shape=jax.ShapeDtypeStruct((5, STACKED, HEAD_SIZE), jnp.bfloat16),
        in_specs=[SMEM] + [VMEM] * 4,
        out_specs=VMEM,
        cost_estimate=pl.CostEstimate(flops=2 << 30, bytes_accessed=4 << 20, transcendentals=0),
        compiler_params=pltpu.CompilerParams(vmem_limit_bytes=12 << 20),
        name="turn_queries",
    )(base, raw, other_raw, cosine, sine)
    rounds = [(row,)]
    states = []

    def step(hop, ahead):
        up, down = rounds[-1][0], rounds[-1][-1]
        if hop == Y // 2:
            up, down = up[: SPAN // 2], down[SPAN // 2 :]
        if ahead is not None:
            up, _ = lax.optimization_barrier((up, ahead))
            down, _ = lax.optimization_barrier((down, ahead))
        rounds.append((shifted(up, 0, 1), shifted(down, 0, -1)))

    step(1, None)
    for hop in range(Y // 2):
        before = states[-1] if states else []
        states.append(
            attend(
                base,
                query,
                rounds[hop],
                (-hop, hop),
                before,
                first=hop == 0,
                diagonal=hop < 3,
            )
        )
        if hop < 3:
            step(hop + 2, states[-1][2])
    *kept, send = attend(base, query, rounds[4], (4, 4), states[-1], last=True, diagonal=False)
    received = lax.ppermute(send, "stretch", SWAP)
    mine = rest(base, query, [*rounds[3], *rounds[4]], ((-3, 1), (3, 1), (4, 2)), kept)
    merged = pl.pallas_call(
        merge_kernel,
        out_shape=jax.ShapeDtypeStruct((2, ROWS, half), jnp.bfloat16),
        in_specs=[SMEM] + [VMEM] * 2,
        out_specs=VMEM,
        compiler_params=pltpu.CompilerParams(vmem_limit_bytes=12 << 20),
        name="merge",
    )(base, mine, received)
    one = lax.ppermute(merged[0], "stretch", back(straight))
    two = lax.ppermute(merged[1], "stretch", back(crossed))
    return jnp.concatenate([jnp.where(low, one, two), jnp.where(low, two, one)], axis=1)


def solution(mesh):
    placed = P(("stretch", "seq"), None)
    return jax.shard_map(
        on_device,
        mesh=mesh,
        in_specs=(placed, placed, placed),
        out_specs=placed,
        check_vma=False,
    )
```
